32 devices in a mesh: dp: 4 (over y, x), row: 2 (over core), col: 4 (over z).
Axes of the slice: x: 2, y: 2, z: 4, core: 2. Of those that a mesh axis runs over, the one named last changes fastest.
Arguments:
- tokens: bfloat16 [3840, 4096], P(('dp', 'col'), 'row'), may hold values from -6 to 6
- hidden_cot: bfloat16 [3840, 14336], P(('dp', 'row'), 'col'), may hold values from -0.09667969 to 0.09667969
- gate_pre: bfloat16 [3840, 14336], P(('dp', 'row'), 'col'), may hold values from -10 to 10
- up_pre: bfloat16 [3840, 14336], P(('dp', 'row'), 'col'), may hold values from -6 to 6
Outputs:
- grad_gate: bfloat16 [2, 2048, 14336], P('row', 'dp', 'col')
The draws below stay inside these ranges and needn't reach their ends.
All inputs are finite; a program needn't handle non-finite values.
Results may differ from the reference program's by a relative error of at most 0.014.
Values may be sent and summed in bfloat16 or wider, within the bound.
No kernel may reach another device: no remote copies, remote signals or barrier semaphores. Data moves between devices by JAX's collectives and lax.ppermute only.
A program may use at most 128 MiB of HBM per device.

```python
import jax
import jax.numpy as jnp
from jax import lax

D = 4096
FF = 14336
GROUP_TOK = 960
TOKENS = 3840
N_DP = 4
N_ROW = 2


def level_of(own_key, shape, split, least, high):
    def one(dim, parts):
        heights = jax.random.uniform(jax.random.fold_in(jax.random.fold_in(own_key, 6), dim), (parts,), jnp.float32, least / len(split), high / len(split))
        return jnp.repeat(jnp.exp(heights), shape[dim] // parts).reshape((-1,) + (1,) * (len(shape) - dim - 1))

    gain = one(*split[0])
    for cut in split[1:]:
        gain = gain * one(*cut)
    return gain


def scatter_about(own_key, dims, deviation, most, shards=(), held_as=jnp.bfloat16):
    drawn = deviation * jax.random.normal(own_key, dims, jnp.float32)
    if shards:
        drawn = drawn * level_of(own_key, dims, shards, -0.22, 0.18)
    return jnp.clip(drawn, -most, most).astype(held_as)


def setup_inputs(seed: int = 0) -> dict:
    seeds = jax.random.split(jax.random.key(seed), 5)
    return {
        "tokens": scatter_about(seeds[0], (TOKENS, D), 1.0, 6.0, ((0, 16), (1, 2))),
        "hidden_cot": scatter_about(seeds[1], (TOKENS, FF), (TOKENS ** -0.5), 0.09667969, ((0, 8), (1, 4))),
        "gate_pre": scatter_about(seeds[2], (TOKENS, FF), 2.0, 10.0, ((0, 8), (1, 4))),
        "up_pre": scatter_about(seeds[3], (TOKENS, FF), 1.0, 6.0, ((0, 8), (1, 4))),
    }


def reference(tokens, hidden_cot, gate_pre, up_pre):
    gate_val = gate_pre.astype(jnp.float32)
    up_val = up_pre.astype(jnp.float32)
    cot_val = hidden_cot.astype(jnp.float32)
    sigma = jax.nn.sigmoid(gate_val)
    gate_grad = (cot_val * up_val * sigma * (1.0 + gate_val * (1.0 - sigma))).astype(jnp.bfloat16)
    tok_groups = tokens.reshape(N_DP, GROUP_TOK, D)
    grad_groups = gate_grad.reshape(N_DP, GROUP_TOK, FF)

    def one_group(total, pair):
        part = jnp.dot(pair[0].T, pair[1], preferred_element_type=jnp.float32).astype(jnp.bfloat16)
        return total + part.astype(jnp.float32), None

    summed, _ = lax.scan(one_group, jnp.zeros((D, FF), jnp.float32), (tok_groups, grad_groups))
    return summed.astype(jnp.bfloat16).reshape(N_ROW, D // N_ROW, FF)
```

```python
import functools
import math

import jax
import jax.numpy as jnp
from jax import lax
from jax.experimental import pallas as pl
from jax.experimental.pallas import tpu as pltpu
from jax.sharding import PartitionSpec as P


CHUNKS = 7
BLOCK = 256
ANY = pl.ANY


def room(*parts):
    return pltpu.CompilerParams(vmem_limit_bytes=sum(math.prod(p) for p in parts) + (3 << 20))


def split(width, parts):
    units = width // 128
    cuts = [units * i // parts * 128 for i in range(parts)] + [width]
    return [(a, b - a) for a, b in zip(cuts, cuts[1:]) if b > a]


def assemble(nz, offsets, *refs):
    place, shards, out, held, sems = refs[0], refs[1:-3], refs[-3], refs[-2], refs[-1]
    size = shards[0].shape[0]
    copies = []
    for i, ref in enumerate(shards):
        group, slot = divmod(i, nz)
        start = pl.multiple_of((group * nz + (place[0] ^ offsets[slot] ^ (place[1] * (nz // 2)))) * size, 16)
        copies.append(pltpu.make_async_copy(ref, held.at[pl.ds(start, size)], sems.at[i]))
        copies[-1].start()
    for copy in copies:
        copy.wait()
    out[...] = held[...].T


def transposed(place, shards, nz, offsets):
    size, tile = shards[0].shape
    total = len(shards) * size
    return pl.pallas_call(
        functools.partial(assemble, nz, offsets),
        out_shape=jax.ShapeDtypeStruct((tile, total), jnp.bfloat16),
        in_specs=[pl.BlockSpec(memory_space=pltpu.SMEM)] + [pl.BlockSpec(memory_space=ANY)] * len(shards),
        out_specs=pl.BlockSpec(memory_space=pltpu.VMEM),
        scratch_shapes=[
            pltpu.VMEM((total, tile), jnp.bfloat16),
            pltpu.SemaphoreType.DMA((len(shards),)),
        ],
        compiler_params=room((total, tile, 6)),
        name="assemble",
    )(place, *shards)


def product(tok, grads, cols, part):
    rows = [ref[:, pl.ds(c + part.start, part.size)] for ref, c in zip(grads, cols)]
    return jnp.dot(tok[...], jnp.concatenate(rows, axis=0), preferred_element_type=jnp.float32)


def parts(width):
    return [pl.ds(c, min(BLOCK, width - c)) for c in range(0, width, BLOCK)]


def send_part(cols, width, tok, *refs):
    *grads, out, value, sems = refs
    stores = []
    for i, part in enumerate(parts(width)):
        value[:, part] = product(tok, grads, cols, part).astype(jnp.bfloat16)
        stores.append(pltpu.make_async_copy(value.at[:, part], out.at[:, part], sems.at[i]))
        stores[-1].start()
    for store in stores:
        store.wait()


def keep_part(cols, col, width, first, tok, *refs):
    *given, out, value, sems = refs
    n = len(cols)
    grads, came = given[:n], given[n:] if first else given[n:-1]
    stores = []
    for i, part in enumerate(parts(width)):
        total = product(tok, grads, cols, part)
        for ref in came:
            total = total + ref[:, part].astype(jnp.float32)
        value[:, part] = total.astype(jnp.bfloat16)
        stores.append(
            pltpu.make_async_copy(
                value.at[:, part], out.at[:, pl.ds(col + part.start, part.size)], sems.at[i]
            )
        )
        stores[-1].start()
    for store in stores:
        store.wait()


def cost(tile, total, width):
    return pl.CostEstimate(
        flops=2 * tile * total * width, bytes_accessed=2 * total * width, transcendentals=0
    )


def send_call(tok, grads, width):
    tile, total = tok.shape
    arrays, cols = zip(*grads)
    return pl.pallas_call(
        functools.partial(send_part, cols, width),
        out_shape=pltpu.HBM((tile, width), jnp.bfloat16),
        in_specs=[pl.BlockSpec(memory_space=pltpu.VMEM)] * (1 + len(arrays)),
        out_specs=pl.BlockSpec(memory_space=pltpu.HBM),
        scratch_shapes=[
            pltpu.VMEM((tile, width), jnp.bfloat16),
            pltpu.SemaphoreType.DMA((-(-width // BLOCK),)),
        ],
        cost_estimate=cost(tile, total, width),
        compiler_params=room((total, width, 4), (tile, total, 2), (tile, width, 8)),
        name="send_part",
    )(tok, *arrays)


def keep_call(tok, grads, came, out, col, width, whole):
    tile, total = tok.shape
    arrays, cols = zip(*grads)
    first = out is None
    given = [tok, *arrays, *came] + ([] if first else [out])
    return pl.pallas_call(
        functools.partial(keep_part, cols, col, width, first),
        out_shape=jax.ShapeDtypeStruct((tile, whole), jnp.bfloat16),
        in_specs=[pl.BlockSpec(memory_space=pltpu.VMEM)] * (1 + len(arrays) + len(came))
        + ([] if first else [pl.BlockSpec(memory_space=ANY)]),
        out_specs=pl.BlockSpec(memory_space=ANY),
        input_output_aliases={} if first else {len(given) - 1: 0},
        scratch_shapes=[
            pltpu.VMEM((tile, width), jnp.bfloat16),
            pltpu.SemaphoreType.DMA((-(-width // BLOCK),)),
        ],
        cost_estimate=cost(tile, total, width),
        compiler_params=room((total, width, 4), (tile, total, 2), (tile, width, 8 + 4 * len(came))),
        name="keep_part",
    )(*given)


def cotangents(cuts, *refs):
    ins, outs, whole = refs[:3], refs[3 : 3 + len(cuts)], refs[3 + len(cuts)]
    held, made, sems, done = refs[4 + len(cuts) :]
    rows = held.shape[2]

    def fetch(j):
        col, width = cuts[j]
        return [
            pltpu.make_async_copy(
                ins[i].at[:, pl.ds(col, width)], held.at[j % 2, i, :, pl.ds(0, width)], sems.at[j % 2, i]
            )
            for i in range(3)
        ]

    def store(j):
        col, width = cuts[j]
        value = made.at[j % 2, :, pl.ds(0, width)]
        return [
            pltpu.make_async_copy(value, outs[j], done.at[j % 2, 0]),
            pltpu.make_async_copy(value, whole.at[:, pl.ds(col - cuts[0][0], width)], done.at[j % 2, 1]),
        ]

    for copy in fetch(0):
        copy.start()
    for j in range(len(cuts)):
        if j + 1 < len(cuts):
            for copy in fetch(j + 1):
                copy.start()
        for copy in fetch(j):
            copy.wait()
        if j >= 2:
            for copy in store(j - 2):
                copy.wait()
        width = cuts[j][1]

        def step(i, _, j=j, width=width):
            part = (pl.ds(pl.multiple_of(i * 32, 32), 32), pl.ds(0, width))
            made[(j % 2, *part)] = gate_cotangent(*(held[(j % 2, n, *part)] for n in range(3)))
            return _

        lax.fori_loop(0, rows // 32, step, 0)
        for copy in store(j):
            copy.start()
    for j in range(max(0, len(cuts) - 2), len(cuts)):
        for copy in store(j):
            copy.wait()


def cotangent_call(arrays, cuts):
    rows = arrays[0].shape[0]
    wide = max(w for _, w in cuts)
    return pl.pallas_call(
        functools.partial(cotangents, cuts),
        out_shape=[pltpu.HBM((rows, w), jnp.bfloat16) for _, w in cuts]
        + [pltpu.HBM((rows, sum(w for _, w in cuts)), jnp.bfloat16)],
        in_specs=[pl.BlockSpec(memory_space=pltpu.HBM)] * 3,
        out_specs=[pl.BlockSpec(memory_space=pltpu.HBM)] * (len(cuts) + 1),
        scratch_shapes=[
            pltpu.VMEM((2, 3, rows, wide), jnp.bfloat16),
            pltpu.VMEM((2, rows, wide), jnp.bfloat16),
            pltpu.SemaphoreType.DMA((2, 3)),
            pltpu.SemaphoreType.DMA((2, 2)),
        ],
        cost_estimate=pl.CostEstimate(flops=20 * rows * wide, bytes_accessed=8 * rows * wide, transcendentals=0),
        compiler_params=room((8, rows, wide, 2)),
        name="cotangents",
    )(*arrays)


def gate_cotangent(hidden_cot, gate_pre, up_pre):
    gate_val = gate_pre.astype(jnp.float32)
    up_val = up_pre.astype(jnp.float32)
    cot_val = hidden_cot.astype(jnp.float32)
    sigma = jax.nn.sigmoid(gate_val)
    return (cot_val * up_val * sigma * (1.0 + gate_val * (1.0 - sigma))).astype(jnp.bfloat16)


def sizes_of(mesh):
    sizes = dict(mesh.shape)
    nx = math.isqrt(sizes["dp"])
    return sizes["dp"] // nx, nx, sizes["row"], sizes["col"]


def on_device(sizes, tokens, hidden_cot, gate_pre, up_pre):
    ny, nx, nrow, nz = sizes
    dp, row, z = lax.axis_index("dp"), lax.axis_index("row"), lax.axis_index("col")
    my_y, my_x = dp // nx, dp % nx
    place = jnp.stack([z, row]).astype(jnp.int32)
    tile = tokens.shape[1] // (ny * nx)
    hidden = hidden_cot.shape[1]

    def over_y(value, k):
        pairs = [(y * nx + x, (y + k) % ny * nx + x) for y in range(ny) for x in range(nx)]
        return lax.ppermute(value, "dp", pairs)

    def over_x(value, m):
        pairs = [(y * nx + x, y * nx + (x + m) % nx) for y in range(ny) for x in range(nx)]
        return lax.ppermute(value, "dp", pairs)

    def over_core(value):
        return lax.ppermute(value, "row", [(i, i ^ 1) for i in range(nrow)])

    def over_z(value):
        slots = {0: value}
        bit = nz // 2
        while bit:
            for s in list(slots):
                slots[s | bit] = lax.ppermute(slots[s], "col", [(i, i ^ bit) for i in range(nz)])
            bit //= 2
        return slots

    def columns(k, m):
        start = ((my_y + k) % ny * nx + (my_x + m) % nx) * tile
        return lax.dynamic_slice(tokens, (0, start), (tokens.shape[0], tile))

    def gathered(m):
        shards, order = [], None
        for k in range(ny):
            mine = columns(k, m)
            slots = over_z(over_y(mine, k) if k else mine)
            order = sorted(slots)
            shards += [slots[s] for s in order]
        return transposed(place, shards, nz, order)

    cuts = split(hidden, CHUNKS)
    arrays = [
        pltpu.with_memory_space_constraint(a, pltpu.HBM) for a in (hidden_cot, gate_pre, up_pre)
    ]
    own, wholes = [], []
    for part in (cuts[:1], cuts[1:]):
        *chunks, whole = cotangent_call(arrays, part)
        own += chunks
        wholes.append((whole, over_core(whole), part[0][0]))
    toks = {m: gathered(m) for m in [*range(1, nx), 0]}
    grads = []
    for j, (c, w) in enumerate(cuts):
        mine, theirs, base = wholes[j > 0]
        pieces = [(mine, c - base), (theirs, c - base)]
        for k in range(1, ny):
            held = over_y(own[j], k)
            pieces += [(held, 0), (over_core(held), 0)]
        grads.append(pieces)
    came = []
    for j, (c, w) in enumerate(cuts):
        came.append([])
        for m in range(1, nx):
            value = send_call(toks[m], grads[j], w)
            came[-1].append(over_x(value, m))
    out = None
    for j, (c, w) in enumerate(cuts):
        out = keep_call(toks[0], grads[j], came[j], out, c, w, hidden)
    return out.reshape(1, *out.shape)


def solution(mesh):
    sizes = sizes_of(mesh)

    def body(*args):
        return on_device(sizes, *args)

    return jax.shard_map(
        body,
        mesh=mesh,
        in_specs=(
            P(("dp", "col"), "row"),
            P(("dp", "row"), "col"),
            P(("dp", "row"), "col"),
            P(("dp", "row"), "col"),
        ),
        out_specs=P("row", "dp", "col"),
        check_vma=False,
    )
```
